128 devices in a mesh: row: 8 (over z_hi, y), col: 8 (over x, core), mp: 2 (over z_lo).
Axes of the slice: x: 4, y: 4, z: 4 (z_hi: 2, z_lo: 2; z = z_hi * 2 + z_lo), core: 2. Of those that a mesh axis runs over, the one named last changes fastest.
Arguments:
- weights: bfloat16 [8, 8, 5, 2304, 1024], P('row', 'col', None, None, 'mp'), may hold values from -6 to 6
- warm_down: bfloat16 [8, 8, 5, 4, 1024], P('row', 'col', None, None, 'mp'), may hold values from -6 to 6
- warm_right: bfloat16 [8, 8, 5, 4, 1024], P('row', 'col', None, None, 'mp'), may hold values from -6 to 6
Outputs:
- new_weights: bfloat16 [8, 8, 5, 2304, 1024], P('row', 'col', None, None, 'mp')
- next_down: float32 [8, 8, 5, 4, 1024], P('row', 'col', None, None, 'mp')
- next_right: float32 [8, 8, 5, 4, 1024], P('row', 'col', None, None, 'mp')
The draws below stay inside these ranges and needn't reach their ends.
All inputs are finite; a program needn't handle non-finite values.
Results may differ from the reference program's by a relative error of at most 0.0085.
Values may be sent and summed in bfloat16 or wider, within the bound.
A program may use at most 128 MiB of HBM per device.

```python
import jax
import jax.numpy as jnp
from jax import lax

D = 2304
KVW = 1024
RANK = 4
LAYERS = 5
ROUNDS = 2
GRID_ROWS = 8
GRID_COLS = 8


def block_levels(key, dims, shards, smallest, high):
    factor_of, own = 1.0, jax.random.fold_in(key, 6)
    for dim, shards_of in shards:
        heights = jnp.exp(jax.random.uniform(jax.random.fold_in(own, dim), (shards_of,), jnp.float32, smallest / len(shards), high / len(shards)))
        factor_of = factor_of * jnp.repeat(heights, dims[dim] // shards_of).reshape([-1 if axis == dim else 1 for axis in range(len(dims))])
    return factor_of


def scatter_about(key, extent, width, bound, split=(), held_as=jnp.bfloat16):
    level = block_levels(key, extent, split, -0.22, 0.18) if split else 1.0
    array = jax.random.normal(key, extent, jnp.float32) * width * level
    return jnp.minimum(jnp.maximum(array, -bound), bound).astype(held_as)


def setup_inputs(seed: int = 0) -> dict:
    arg_keys = jax.random.split(jax.random.key(seed), 4)
    weights = scatter_about(arg_keys[0], (GRID_ROWS, GRID_COLS, LAYERS, D, KVW), 1.0, 6.0, ((0, 8), (1, 8), (4, 2)))
    warm_down = scatter_about(arg_keys[1], (GRID_ROWS, GRID_COLS, LAYERS, RANK, KVW), 1.0, 6.0, ((0, 8), (1, 8), (4, 2)))
    warm_right = scatter_about(arg_keys[2], (GRID_ROWS, GRID_COLS, LAYERS, RANK, KVW), 1.0, 6.0, ((0, 8), (1, 8), (4, 2)))
    return {"weights": weights, "warm_down": warm_down, "warm_right": warm_right}


step_size = 0.2
epsilon = 1e-06

def orthonormal(vectors):
    basis = []
    for column in range(vectors.shape[-2]):
        source = vectors[..., column, :]
        update = source
        for earlier in basis:
            update = update - lax.optimization_barrier(jnp.sum(source * earlier, axis=-1, keepdims=True)) * earlier
        basis.append(update / jnp.sqrt(lax.optimization_barrier(jnp.sum(update * update, axis=-1, keepdims=True)) + epsilon))
    return jnp.stack(basis, axis=-2)

def forward_products(layer_x, factors):

    def single(operands):
        return jnp.dot(operands[1], operands[0].T, preferred_element_type=jnp.float32)
    return lax.map(single, (layer_x, factors))

def backward_products(layer_x, basis):

    def single(operands):
        return jnp.dot(operands[1], operands[0], preferred_element_type=jnp.float32)
    return lax.map(single, (layer_x, basis))

def apply_update(layer_x, basis, factors):

    def single(triple):
        correction = jnp.dot(triple[1].T, triple[2], preferred_element_type=jnp.float32)
        return (triple[0].astype(jnp.float32) - step_size * correction).astype(jnp.bfloat16)
    return lax.map(single, (layer_x, basis, factors))

def one_round(layer_x, down_q, right_q):
    node_count = GRID_ROWS * GRID_COLS
    flat_x = layer_x.reshape(node_count, D, KVW)

    def to_grid(values):
        return values.reshape(GRID_ROWS, GRID_COLS, values.shape[1], values.shape[2])

    def to_flat(values):
        return values.reshape(node_count, values.shape[2], values.shape[3])
    stacked = jnp.concatenate([down_q, right_q, jnp.roll(down_q, 1, 0), jnp.roll(right_q, 1, 1)], axis=2)
    forward = to_grid(forward_products(flat_x, to_flat(stacked)))
    down_diff = forward[:, :, :RANK] - jnp.roll(forward[:, :, 2 * RANK:3 * RANK], -1, 0)
    right_diff = forward[:, :, RANK:2 * RANK] - jnp.roll(forward[:, :, 3 * RANK:], -1, 1)
    down_p = orthonormal(down_diff).astype(jnp.bfloat16)
    right_p = orthonormal(right_diff).astype(jnp.bfloat16)
    basis = jnp.concatenate([down_p, right_p, jnp.roll(down_p, 1, 0), jnp.roll(right_p, 1, 1)], axis=2)
    backward = to_grid(backward_products(flat_x, to_flat(basis)))
    down_c = backward[:, :, :RANK] - jnp.roll(backward[:, :, 2 * RANK:3 * RANK], -1, 0)
    right_c = backward[:, :, RANK:2 * RANK] - jnp.roll(backward[:, :, 3 * RANK:], -1, 1)
    down_next = down_c.astype(jnp.bfloat16)
    right_next = right_c.astype(jnp.bfloat16)
    own_basis = jnp.concatenate([down_p, right_p, -jnp.roll(down_p, 1, 0), -jnp.roll(right_p, 1, 1)], axis=2)
    own_factors = jnp.concatenate([down_next, right_next, jnp.roll(down_next, 1, 0), jnp.roll(right_next, 1, 1)], axis=2)
    new_x = apply_update(flat_x, to_flat(own_basis), to_flat(own_factors)).reshape(layer_x.shape)
    return (new_x, down_next, right_next, down_c, right_c)

def reference(weights, warm_down, warm_right):
    new_layers = []
    downs = []
    rights = []
    for level_index in range(LAYERS):
        layer_x = weights[:, :, level_index]
        down_q = warm_down[:, :, level_index]
        right_q = warm_right[:, :, level_index]
        down_c = jnp.zeros(down_q.shape, jnp.float32)
        right_c = jnp.zeros(right_q.shape, jnp.float32)
        for repeat in range(ROUNDS):
            layer_x, down_q, right_q, down_c, right_c = one_round(layer_x, down_q, right_q)
        new_layers.append(layer_x)
        downs.append(down_c)
        rights.append(right_c)
    return (jnp.stack(new_layers, 2), jnp.stack(downs, 2), jnp.stack(rights, 2))
```

```python
import functools

import jax
import jax.numpy as jnp
from jax import lax
from jax.experimental import pallas as pl
from jax.experimental.pallas import tpu as pltpu
from jax.sharding import PartitionSpec as P

STEP = 0.2
EPS = 1e-06
MESH = pl.DeviceIdType.MESH
F32, BF16 = jnp.float32, jnp.bfloat16
NT = (((1,), (1,)), ((), ()))
NN = (((1,), (0,)), ((), ()))
TN = (((0,), (0,)), ((), ()))


def low_half(shape):
    return lax.broadcasted_iota(jnp.int32, shape, len(shape) - 2) % 8 < 4


def dot(a, b, dims):
    return lax.dot_general(a, b, dims, preferred_element_type=F32)


def orthonormal(total, others, chunks):
    sums = [None] * 4
    for j in range(chunks):
        v = total(j) - others(j)
        for s in range(4):
            term = v * (pltpu.roll(v, s, 1) if s else v)
            sums[s] = term if sums[s] is None else sums[s] + term
    gram = []
    for s in range(4):
        g = jnp.broadcast_to(jnp.sum(sums[s], axis=-1, keepdims=True), sums[s].shape)
        gram.append(g + pltpu.roll(g, 4, 1))

    def at(i, j):
        g = gram[i - j]
        return pltpu.roll(g, 8 - i, 1) if i else g

    g = [[at(i, j) for j in range(i + 1)] for i in range(4)]
    c = [[lax.rsqrt(g[0][0] + EPS)]]
    for k in range(1, 4):
        along = [sum(c[j][i] * g[k][i] for i in range(j + 1)) for j in range(k)]
        m = [-sum(along[j] * c[j][i] for j in range(i, k)) for i in range(k)]
        square = g[k][k]
        for i in range(k):
            inner = 2.0 * g[k][i] + m[i] * g[i][i]
            for j in range(i):
                inner = inner + 2.0 * (m[j] * g[i][j])
            square = square + m[i] * inner
        norm = lax.rsqrt(jnp.maximum(square, 0.0) + EPS)
        c.append([norm * x for x in m] + [norm])
    row = lax.broadcasted_iota(jnp.int32, g[0][0].shape, 1) % 4
    columns = []
    for s in range(4):
        column = jnp.zeros(g[0][0].shape, F32)
        for k in range(s, 4):
            value = c[k][k - s]
            column = jnp.where(row == k, pltpu.roll(value, k, 1) if k else value, column)
        columns.append(column)
    out = []
    for j in range(chunks):
        v = total(j) - others(j)
        p = columns[0] * v
        for s in range(1, 4):
            p = p + columns[s] * pltpu.roll(v, s, 1)
        out.append(p)
    return out


def exchange_kernel(
    w_hbm, wd_hbm, wr_hbm, p_ref, f_ref, cd_ref, cr_ref,
    w, warm, total, send1, recv1, send2, recv2, back, send3, recv3,
    w_sem, warm_sem, warm_send, warm_recv, s1, r1, s2, r2, s3, r3,
):
    layers, depth, width = w.shape
    half = depth // 2
    chunks = half // 128
    row, col, mp = lax.axis_index("row"), lax.axis_index("col"), lax.axis_index("mp")
    down, up = lax.rem(row + 1, 8), lax.rem(row + 7, 8)
    right, left = lax.rem(col + 1, 8), lax.rem(col + 7, 8)
    cross_down = lax.rem(mp + lax.div(lax.rem(row, 4), 3), 2)
    cross_up = lax.rem(mp + lax.div(lax.rem(row + 3, 4), 3), 2)
    partner = (row, col, 1 - mp)
    straight = [(down, col, mp), (row, right, mp), (up, col, mp), (row, left, mp)]
    crossed = [(down, col, cross_down), (row, right, mp), (up, col, cross_up), (row, left, mp)]

    barrier = pltpu.get_barrier_semaphore()
    for device in [partner] + straight + [crossed[0], crossed[2]]:
        pl.semaphore_signal(barrier, inc=1, device_id=device, device_id_type=MESH)

    def warm_load(e):
        return pltpu.make_async_copy([wd_hbm, wr_hbm][e].at[0, 0], warm.at[e], warm_sem.at[e])

    def w_load(l):
        return pltpu.make_async_copy(w_hbm.at[0, 0, l], w.at[l], w_sem.at[l])

    for e in range(2):
        warm_load(e).start()
    for l in range(layers):
        w_load(l).start()

    def warm_copy(e):
        return pltpu.make_async_remote_copy(
            warm.at[e], warm.at[e + 2], warm_send.at[e], warm_recv.at[e], device_id=straight[e], device_id_type=MESH)

    def mp_copy(r, l, e, n):
        return pltpu.make_async_remote_copy(
            send1.at[r, l, pl.ds(e, n)], recv1.at[r, l, pl.ds(e, n)], s1.at[r, l, e // 2], r1.at[r, l, e // 2],
            device_id=partner, device_id_type=MESH)

    def sum_copy(r, l, e):
        return pltpu.make_async_remote_copy(
            send2.at[r, l, e], recv2.at[r, l, (e + 2) % 4], s2.at[r, l], r2.at[r, l],
            device_id=crossed[e], device_id_type=MESH)

    def sums_copy(r, l):
        return pltpu.make_async_remote_copy(
            send2.at[r, l], recv2.at[r, l], s2.at[r, l], r2.at[r, l], device_id=partner, device_id_type=MESH)

    def back_copy(r, l, e):
        return pltpu.make_async_remote_copy(
            send3.at[r, l, e], recv3.at[r, l, (e + 2) % 4], s3.at[r, l], r3.at[r, l],
            device_id=straight[e], device_id_type=MESH)

    def backs_copy(r, l):
        return pltpu.make_async_remote_copy(
            send3.at[r, l], recv3.at[r, l], s3.at[r, l], r3.at[r, l], device_id=partner, device_id_type=MESH)

    def forward(factors, l):
        first = dot(factors, w[l, :half], NT)
        second = dot(factors, w[l, half:], NT)
        return jnp.where(low_half(first.shape), first, second)

    def first_forward(l, e):
        pieces = []
        for i in (e, e + 1):
            rows = warm[i, l].astype(F32)
            pieces += [rows, rows]
        product = forward(jnp.concatenate(pieces, axis=0).astype(BF16), l)
        product = product.reshape(2, 8, half)
        total[l, e:e + 2] = product
        send1[0, l, e:e + 2] = product.astype(BF16)
        mp_copy(0, l, e, 2).start()

    def own_edges(l, _):
        w_load(l).wait()
        first_forward(l, 0)

    def other_edges(l, _):
        first_forward(l, 2)

    def add_up(r, l, e, n):
        mp_copy(r, l, e, n).wait_recv()
        value = total[l, e:e + n] + recv1[r, l, e:e + n].astype(F32)
        total[l, e:e + n] = value
        send2[r, l, e:e + n] = value.astype(BF16)
        for i in range(e, e + n):
            sum_copy(r, l, i).start()

    def backward(r, l):
        sums_copy(r, l).wait_recv()

        def mine(j):
            return total[l, :, :, 128 * j:128 * (j + 1)]

        def theirs(j):
            return recv2[r, l, :, :, 128 * j:128 * (j + 1)].astype(F32)

        for j, piece in enumerate(orthonormal(mine, theirs, chunks)):
            p_ref[l, 32 * r:32 * (r + 1), 128 * j:128 * (j + 1)] = piece.reshape(32, 128).astype(BF16)
        basis = p_ref[l, 32 * r:32 * (r + 1)]
        first = dot(basis, w[l, :half], NN)
        second = dot(basis, w[l, half:], NN)
        parts = jnp.where(low_half(first.shape), first, second)
        if r:
            overlap = dot(basis, p_ref[l, :32], NT)
            same = low_half(overlap.shape) == (lax.broadcasted_iota(jnp.int32, overlap.shape, 1) % 8 < 4)
            overlap = jnp.where(same, overlap, 0.0).astype(BF16)
            parts = parts - STEP * dot(overlap, f_ref[l, :32], NN)
        parts = parts.reshape(4, 8, width)
        value = parts + pltpu.roll(parts, 4, 1)
        back[l] = value
        send3[r, l] = value.astype(BF16)
        for e in range(4):
            back_copy(r, l, e).start()

    def combine(r, l):
        backs_copy(r, l).wait_recv()
        value = back[l] + recv3[r, l].astype(F32)
        factors = value.reshape(32, width).astype(BF16)
        f_ref[l, 32 * r:32 * (r + 1)] = factors
        return value, factors

    def second_forward(l, _):
        _, factors = combine(0, l)
        product = forward(factors, l)
        overlap = dot(factors, factors, NT)
        same = low_half(overlap.shape) == (lax.broadcasted_iota(jnp.int32, overlap.shape, 1) % 8 < 4)
        overlap = jnp.where(same, overlap, 0.0).astype(BF16)
        product = product - STEP * dot(overlap, p_ref[l, :32], NN)
        product = product.reshape(4, 8, half)
        total[l] = product
        send1[1, l] = product.astype(BF16)
        mp_copy(1, l, 0, 4).start()

    def last(l, _):
        value, _ = combine(1, l)
        cd_ref[l] = value[0, :4]
        cr_ref[l] = value[1, :4]

    def each(function):
        lax.fori_loop(0, layers, lambda l, carry: (function(l, None), carry)[1], 0)

    for e in range(2):
        warm_load(e).wait()
    pl.semaphore_wait(barrier, 7)
    for e in range(2):
        warm_copy(e).start()
    each(own_edges)
    for e in range(2):
        warm_copy(e).wait_recv()
    each(other_edges)
    each(lambda l, _: (add_up(0, l, 0, 2), add_up(0, l, 2, 2)))
    each(lambda l, _: backward(0, l))
    each(second_forward)
    each(lambda l, _: add_up(1, l, 0, 4))
    each(lambda l, _: backward(1, l))
    each(last)
    for e in range(2):
        warm_copy(e).wait_send()

    def drain(l, _):
        mp_copy(0, l, 0, 2).wait_send()
        mp_copy(0, l, 2, 2).wait_send()
        mp_copy(1, l, 0, 4).wait_send()
        for r in range(2):
            sums_copy(r, l).wait_send()
            backs_copy(r, l).wait_send()

    each(drain)


def exchange(weights, warm_down, warm_right):
    layers, depth, width = weights.shape[2:]
    half = depth // 2
    vmem = pl.BlockSpec(memory_space=pltpu.VMEM)
    hbm = pl.BlockSpec(memory_space=pltpu.HBM)
    dma = pltpu.SemaphoreType.DMA
    return pl.pallas_call(
        exchange_kernel,
        out_shape=(
            jax.ShapeDtypeStruct((layers, 64, half), BF16),
            jax.ShapeDtypeStruct((layers, 64, width), BF16),
            jax.ShapeDtypeStruct((layers, 4, width), F32),
            jax.ShapeDtypeStruct((layers, 4, width), F32),
        ),
        in_specs=[hbm] * 3,
        out_specs=(vmem,) * 4,
        scratch_shapes=[
            pltpu.VMEM((layers, depth, width), BF16),
            pltpu.VMEM((4, layers, 4, width), BF16),
            pltpu.VMEM((layers, 4, 8, half), F32),
            pltpu.VMEM((2, layers, 4, 8, half), BF16),
            pltpu.VMEM((2, layers, 4, 8, half), BF16),
            pltpu.VMEM((2, layers, 4, 8, half), BF16),
            pltpu.VMEM((2, layers, 4, 8, half), BF16),
            pltpu.VMEM((layers, 4, 8, width), F32),
            pltpu.VMEM((2, layers, 4, 8, width), BF16),
            pltpu.VMEM((2, layers, 4, 8, width), BF16),
            dma((layers,)), dma((2,)), dma((2,)), dma((2,)),
            dma((2, layers, 2)), dma((2, layers, 2)),
            dma((2, layers)), dma((2, layers)), dma((2, layers)), dma((2, layers)),
        ],
        compiler_params=pltpu.CompilerParams(collective_id=0, has_side_effects=True, vmem_limit_bytes=48 * 2**20),
        name="exchange",
    )(weights, warm_down, warm_right)


def update_kernel(w_ref, p_ref, f_ref, cd_ref, cr_ref, out_ref, down_ref, right_ref):
    keep = low_half(f_ref.shape[1:]) == (pl.program_id(1) == 0)
    factors = jnp.where(keep, f_ref[0], jnp.zeros_like(f_ref[0]))
    correction = dot(p_ref[0], factors, TN)
    out_ref[0, 0, 0] = (w_ref[0, 0, 0].astype(F32) - STEP * correction).astype(BF16)
    down_ref[0, 0] = cd_ref[...]
    right_ref[0, 0] = cr_ref[...]


def update(weights, basis, factors, down, right):
    layers, depth, width = weights.shape[2:]
    half = depth // 2
    block = pl.BlockSpec((1, 1, 1, half, width), lambda l, h: (0, 0, l, h, 0))
    whole = pl.BlockSpec((layers, 4, width), lambda l, h: (0, 0, 0))
    placed = pl.BlockSpec((1, 1, layers, 4, width), lambda l, h: (0, 0, 0, 0, 0))
    return pl.pallas_call(
        update_kernel,
        grid=(layers, 2),
        out_shape=(
            jax.ShapeDtypeStruct(weights.shape, BF16),
            jax.ShapeDtypeStruct((1, 1, layers, 4, width), F32),
            jax.ShapeDtypeStruct((1, 1, layers, 4, width), F32),
        ),
        in_specs=[
            block,
            pl.BlockSpec((1, 64, half), lambda l, h: (l, 0, 0)),
            pl.BlockSpec((1, 64, width), lambda l, h: (l, 0, 0)),
            whole,
            whole,
        ],
        out_specs=(block, placed, placed),
        name="update",
    )(weights, basis, factors, down, right)


def body(weights, warm_down, warm_right):
    return update(weights, *exchange(weights, warm_down, warm_right))


def solution(mesh):
    placed = (P("row", "col", None, None, "mp"),) * 3
    return jax.shard_map(body, mesh=mesh, in_specs=placed, out_specs=placed, check_vma=False)
```

```python
import functools

import jax
import jax.numpy as jnp
from jax import lax
from jax.experimental import pallas as pl
from jax.experimental.pallas import tpu as pltpu
from jax.sharding import PartitionSpec as P

STEP = 0.2
EPS = 1e-06
MESH = pl.DeviceIdType.MESH
F32, BF16 = jnp.float32, jnp.bfloat16
NT = (((1,), (1,)), ((), ()))
NN = (((1,), (0,)), ((), ()))
TN = (((0,), (0,)), ((), ()))


def low_half(shape):
    return lax.broadcasted_iota(jnp.int32, shape, len(shape) - 2) % 8 < 4


def dot(a, b, dims):
    return lax.dot_general(a, b, dims, preferred_element_type=F32)


def orthonormal(total, others, chunks):
    sums = [None] * 4
    for j in range(chunks):
        v = total(j) - others(j)
        for s in range(4):
            term = v * (pltpu.roll(v, s, 1) if s else v)
            sums[s] = term if sums[s] is None else sums[s] + term
    gram = []
    for s in range(4):
        g = jnp.broadcast_to(jnp.sum(sums[s], axis=-1, keepdims=True), sums[s].shape)
        gram.append(g + pltpu.roll(g, 4, 1))

    def at(i, j):
        g = gram[i - j]
        return pltpu.roll(g, 8 - i, 1) if i else g

    g = [[at(i, j) for j in range(i + 1)] for i in range(4)]
    c = [[lax.rsqrt(g[0][0] + EPS)]]
    for k in range(1, 4):
        along = [sum(c[j][i] * g[k][i] for i in range(j + 1)) for j in range(k)]
        m = [-sum(along[j] * c[j][i] for j in range(i, k)) for i in range(k)]
        square = g[k][k]
        for i in range(k):
            inner = 2.0 * g[k][i] + m[i] * g[i][i]
            for j in range(i):
                inner = inner + 2.0 * (m[j] * g[i][j])
            square = square + m[i] * inner
        norm = lax.rsqrt(jnp.maximum(square, 0.0) + EPS)
        c.append([norm * x for x in m] + [norm])
    row = lax.broadcasted_iota(jnp.int32, g[0][0].shape, 1) % 4
    columns = []
    for s in range(4):
        column = jnp.zeros(g[0][0].shape, F32)
        for k in range(s, 4):
            value = c[k][k - s]
            column = jnp.where(row == k, pltpu.roll(value, k, 1) if k else value, column)
        columns.append(column)
    out = []
    for j in range(chunks):
        v = total(j) - others(j)
        p = columns[0] * v
        for s in range(1, 4):
            p = p + columns[s] * pltpu.roll(v, s, 1)
        out.append(p)
    return out


def exchange_kernel(
    w_hbm, wd_hbm, wr_hbm, w, cd_ref, cr_ref,
    p_ref, f_ref, warm, total, send1, recv1, send2, recv2, back, send3, recv3,
    w_sem, warm_sem, warm_send, warm_recv, s1, r1, s2, r2, s3, r3,
):
    layers, depth, width = w.shape
    half = depth // 2
    chunks = half // 128
    row, col, mp = lax.axis_index("row"), lax.axis_index("col"), lax.axis_index("mp")
    down, up = lax.rem(row + 1, 8), lax.rem(row + 7, 8)
    right, left = lax.rem(col + 1, 8), lax.rem(col + 7, 8)
    cross_down = lax.rem(mp + lax.div(lax.rem(row, 4), 3), 2)
    cross_up = lax.rem(mp + lax.div(lax.rem(row + 3, 4), 3), 2)
    partner = (row, col, 1 - mp)
    straight = [(down, col, mp), (row, right, mp), (up, col, mp), (row, left, mp)]
    crossed = [(down, col, cross_down), (row, right, mp), (up, col, cross_up), (row, left, mp)]

    barrier = pltpu.get_barrier_semaphore()
    for device in [partner] + straight + [crossed[0], crossed[2]]:
        pl.semaphore_signal(barrier, inc=1, device_id=device, device_id_type=MESH)

    def warm_load(e):
        return pltpu.make_async_copy([wd_hbm, wr_hbm][e].at[0, 0], warm.at[e], warm_sem.at[e])

    def w_load(l):
        return pltpu.make_async_copy(w_hbm.at[0, 0, l], w.at[l], w_sem.at[l])

    for e in range(2):
        warm_load(e).start()
    for l in range(layers):
        w_load(l).start()

    def warm_copy(e):
        return pltpu.make_async_remote_copy(
            warm.at[e], warm.at[e + 2], warm_send.at[e], warm_recv.at[e], device_id=straight[e], device_id_type=MESH)

    def mp_copy(r, l, e, n):
        return pltpu.make_async_remote_copy(
            send1.at[r, l, pl.ds(e, n)], recv1.at[r, l, pl.ds(e, n)], s1.at[r, l, e // 2], r1.at[r, l, e // 2],
            device_id=partner, device_id_type=MESH)

    def sum_copy(r, l, e):
        return pltpu.make_async_remote_copy(
            send2.at[r, l, e], recv2.at[r, l, (e + 2) % 4], s2.at[r, l], r2.at[r, l],
            device_id=crossed[e], device_id_type=MESH)

    def sums_copy(r, l):
        return pltpu.make_async_remote_copy(
            send2.at[r, l], recv2.at[r, l], s2.at[r, l], r2.at[r, l], device_id=partner, device_id_type=MESH)

    def back_copy(r, l, e):
        return pltpu.make_async_remote_copy(
            send3.at[r, l, e], recv3.at[r, l, (e + 2) % 4], s3.at[r, l], r3.at[r, l],
            device_id=straight[e], device_id_type=MESH)

    def backs_copy(r, l):
        return pltpu.make_async_remote_copy(
            send3.at[r, l], recv3.at[r, l], s3.at[r, l], r3.at[r, l], device_id=partner, device_id_type=MESH)

    def forward(factors, l):
        first = dot(factors, w[l, :half], NT)
        second = dot(factors, w[l, half:], NT)
        return jnp.where(low_half(first.shape), first, second)

    def first_forward(l, e):
        pieces = []
        for i in (e, e + 1):
            rows = warm[i, l].astype(F32)
            pieces += [rows, rows]
        product = forward(jnp.concatenate(pieces, axis=0).astype(BF16), l)
        product = product.reshape(2, 8, half)
        total[l, e:e + 2] = product
        send1[0, l, e:e + 2] = product.astype(BF16)
        mp_copy(0, l, e, 2).start()

    def own_edges(l, _):
        w_load(l).wait()
        first_forward(l, 0)

    def other_edges(l, _):
        first_forward(l, 2)

    def add_up(r, l, e, n):
        mp_copy(r, l, e, n).wait_recv()
        value = total[l, e:e + n] + recv1[r, l, e:e + n].astype(F32)
        total[l, e:e + n] = value
        send2[r, l, e:e + n] = value.astype(BF16)
        for i in range(e, e + n):
            sum_copy(r, l, i).start()

    def backward(r, l):
        sums_copy(r, l).wait_recv()

        def mine(j):
            return total[l, :, :, 128 * j:128 * (j + 1)]

        def theirs(j):
            return recv2[r, l, :, :, 128 * j:128 * (j + 1)].astype(F32)

        for j, piece in enumerate(orthonormal(mine, theirs, chunks)):
            p_ref[l, 32 * r:32 * (r + 1), 128 * j:128 * (j + 1)] = piece.reshape(32, 128).astype(BF16)
        basis = p_ref[l, 32 * r:32 * (r + 1)]
        first = dot(basis, w[l, :half], NN)
        second = dot(basis, w[l, half:], NN)
        parts = jnp.where(low_half(first.shape), first, second)
        if r:
            overlap = dot(basis, p_ref[l, :32], NT)
            same = low_half(overlap.shape) == (lax.broadcasted_iota(jnp.int32, overlap.shape, 1) % 8 < 4)
            overlap = jnp.where(same, overlap, 0.0).astype(BF16)
            parts = parts - STEP * dot(overlap, f_ref[l, :32], NN)
        parts = parts.reshape(4, 8, width)
        value = parts + pltpu.roll(parts, 4, 1)
        back[l] = value
        send3[r, l] = value.astype(BF16)
        for e in range(4):
            back_copy(r, l, e).start()

    def combine(r, l):
        backs_copy(r, l).wait_recv()
        value = back[l] + recv3[r, l].astype(F32)
        factors = value.reshape(32, width).astype(BF16)
        f_ref[l, 32 * r:32 * (r + 1)] = factors
        return value, factors

    def second_forward(l, _):
        _, factors = combine(0, l)
        product = forward(factors, l)
        overlap = dot(factors, factors, NT)
        same = low_half(overlap.shape) == (lax.broadcasted_iota(jnp.int32, overlap.shape, 1) % 8 < 4)
        overlap = jnp.where(same, overlap, 0.0).astype(BF16)
        product = product - STEP * dot(overlap, p_ref[l, :32], NN)
        product = product.reshape(4, 8, half)
        total[l] = product
        send1[1, l] = product.astype(BF16)
        mp_copy(1, l, 0, 4).start()

    def last(l, _):
        value, _ = combine(1, l)
        cd_ref[l] = value[0, :4]
        cr_ref[l] = value[1, :4]
        factors = f_ref[l]
        low = low_half(factors.shape)
        for h in range(2):
            kept = jnp.where(low == (h == 0), factors, jnp.zeros_like(factors))
            rows = pl.ds(half * h, half)
            w[l, rows] = (w[l, rows].astype(F32) - STEP * dot(p_ref[l], kept, TN)).astype(BF16)

    def each(function):
        lax.fori_loop(0, layers, lambda l, carry: (function(l, None), carry)[1], 0)

    for e in range(2):
        warm_load(e).wait()
    pl.semaphore_wait(barrier, 7)
    for e in range(2):
        warm_copy(e).start()
    each(own_edges)
    for e in range(2):
        warm_copy(e).wait_recv()
    each(other_edges)
    each(lambda l, _: (add_up(0, l, 0, 2), add_up(0, l, 2, 2)))
    each(lambda l, _: backward(0, l))
    each(second_forward)
    each(lambda l, _: add_up(1, l, 0, 4))
    each(lambda l, _: backward(1, l))
    each(last)
    for e in range(2):
        warm_copy(e).wait_send()

    def drain(l, _):
        mp_copy(0, l, 0, 2).wait_send()
        mp_copy(0, l, 2, 2).wait_send()
        mp_copy(1, l, 0, 4).wait_send()
        for r in range(2):
            sums_copy(r, l).wait_send()
            backs_copy(r, l).wait_send()

    each(drain)


def exchange(weights, warm_down, warm_right):
    layers, depth, width = weights.shape[2:]
    half = depth // 2
    vmem = pl.BlockSpec(memory_space=pltpu.VMEM)
    hbm = pl.BlockSpec(memory_space=pltpu.HBM)
    dma = pltpu.SemaphoreType.DMA
    return pl.pallas_call(
        exchange_kernel,
        out_shape=(
            jax.ShapeDtypeStruct((layers, depth, width), BF16),
            jax.ShapeDtypeStruct((layers, 4, width), F32),
            jax.ShapeDtypeStruct((layers, 4, width), F32),
        ),
        in_specs=[hbm] * 3,
        out_specs=(vmem,) * 3,
        scratch_shapes=[
            pltpu.VMEM((layers, 64, half), BF16),
            pltpu.VMEM((layers, 64, width), BF16),
            pltpu.VMEM((4, layers, 4, width), BF16),
            pltpu.VMEM((layers, 4, 8, half), F32),
            pltpu.VMEM((2, layers, 4, 8, half), BF16),
            pltpu.VMEM((2, layers, 4, 8, half), BF16),
            pltpu.VMEM((2, layers, 4, 8, half), BF16),
            pltpu.VMEM((2, layers, 4, 8, half), BF16),
            pltpu.VMEM((layers, 4, 8, width), F32),
            pltpu.VMEM((2, layers, 4, 8, width), BF16),
            pltpu.VMEM((2, layers, 4, 8, width), BF16),
            dma((layers,)), dma((2,)), dma((2,)), dma((2,)),
            dma((2, layers, 2)), dma((2, layers, 2)),
            dma((2, layers)), dma((2, layers)), dma((2, layers)), dma((2, layers)),
        ],
        compiler_params=pltpu.CompilerParams(collective_id=0, has_side_effects=True, vmem_limit_bytes=20 * 2**20),
        name="exchange",
    )(weights, warm_down, warm_right)


def write_kernel(w_ref, down_ref, right_ref, w_out, down_out, right_out, sems):
    layers = w_ref.shape[0]
    copies = [
        pltpu.make_async_copy(down_ref, down_out.at[0, 0], sems.at[0]),
        pltpu.make_async_copy(right_ref, right_out.at[0, 0], sems.at[1]),
    ]
    copies += [pltpu.make_async_copy(w_ref.at[l], w_out.at[0, 0, l], sems.at[2 + l]) for l in range(layers)]
    for copy in copies:
        copy.start()
    for copy in copies:
        copy.wait()


def write(w, down, right):
    layers, depth, width = w.shape
    vmem = pl.BlockSpec(memory_space=pltpu.VMEM)
    hbm = pl.BlockSpec(memory_space=pltpu.HBM)
    return pl.pallas_call(
        write_kernel,
        out_shape=(
            jax.ShapeDtypeStruct((1, 1, layers, depth, width), BF16),
            jax.ShapeDtypeStruct((1, 1, layers, 4, width), F32),
            jax.ShapeDtypeStruct((1, 1, layers, 4, width), F32),
        ),
        in_specs=[vmem] * 3,
        out_specs=(hbm,) * 3,
        scratch_shapes=[pltpu.SemaphoreType.DMA((2 + layers,))],
        compiler_params=pltpu.CompilerParams(vmem_limit_bytes=2**20),
        name="write",
    )(w, down, right)


def body(weights, warm_down, warm_right):
    held = [pltpu.with_memory_space_constraint(x, pltpu.HBM) for x in (weights, warm_down, warm_right)]
    return write(*exchange(*held))


def solution(mesh):
    placed = (P("row", "col", None, None, "mp"),) * 3
    return jax.shard_map(body, mesh=mesh, in_specs=placed, out_specs=placed, check_vma=False)
```

```python
import functools

import jax
import jax.numpy as jnp
from jax import lax
from jax.experimental import pallas as pl
from jax.experimental.pallas import tpu as pltpu
from jax.sharding import PartitionSpec as P

STEP = 0.2
EPS = 1e-06
MESH = pl.DeviceIdType.MESH
F32, BF16 = jnp.float32, jnp.bfloat16
NT = (((1,), (1,)), ((), ()))
NN = (((1,), (0,)), ((), ()))
TN = (((0,), (0,)), ((), ()))


def low_half(shape):
    return lax.broadcasted_iota(jnp.int32, shape, len(shape) - 2) % 8 < 4


def dot(a, b, dims):
    return lax.dot_general(a, b, dims, preferred_element_type=F32)


def orthonormal(total, others, chunks):
    sums = [None] * 4
    for j in range(chunks):
        v = total(j) - others(j)
        for s in range(4):
            term = v * (pltpu.roll(v, s, 1) if s else v)
            sums[s] = term if sums[s] is None else sums[s] + term
    gram = []
    for s in range(4):
        g = jnp.broadcast_to(jnp.sum(sums[s], axis=-1, keepdims=True), sums[s].shape)
        gram.append(g + pltpu.roll(g, 4, 1))

    def at(i, j):
        g = gram[i - j]
        return pltpu.roll(g, 8 - i, 1) if i else g

    g = [[at(i, j) for j in range(i + 1)] for i in range(4)]
    c = [[lax.rsqrt(g[0][0] + EPS)]]
    for k in range(1, 4):
        along = [sum(c[j][i] * g[k][i] for i in range(j + 1)) for j in range(k)]
        m = [-sum(along[j] * c[j][i] for j in range(i, k)) for i in range(k)]
        square = g[k][k]
        for i in range(k):
            inner = 2.0 * g[k][i] + m[i] * g[i][i]
            for j in range(i):
                inner = inner + 2.0 * (m[j] * g[i][j])
            square = square + m[i] * inner
        norm = lax.rsqrt(jnp.maximum(square, 0.0) + EPS)
        c.append([norm * x for x in m] + [norm])
    row = lax.broadcasted_iota(jnp.int32, g[0][0].shape, 1) % 4
    columns = []
    for s in range(4):
        column = jnp.zeros(g[0][0].shape, F32)
        for k in range(s, 4):
            value = c[k][k - s]
            column = jnp.where(row == k, pltpu.roll(value, k, 1) if k else value, column)
        columns.append(column)
    out = []
    for j in range(chunks):
        v = total(j) - others(j)
        p = columns[0] * v
        for s in range(1, 4):
            p = p + columns[s] * pltpu.roll(v, s, 1)
        out.append(p)
    return out


def updated(w, basis, factors, h):
    low = low_half(factors.shape)
    kept = jnp.where(low == (h == 0), factors, jnp.zeros_like(factors))
    return (w.astype(F32) - STEP * dot(basis, kept, TN)).astype(BF16)


def exchange_kernel(
    w_hbm, wd_hbm, wr_hbm, w, p_ref, f_ref, cd_ref, cr_ref,
    wt, warm, total, send1, recv1, send2, recv2, back, send3, recv3,
    w_sem, warm_sem, warm_send, warm_recv, s1, r1, s2, r2, s3, r3,
):
    layers, depth, width = w.shape
    half = depth // 2
    chunks = half // 128
    row, col, mp = lax.axis_index("row"), lax.axis_index("col"), lax.axis_index("mp")
    down, up = lax.rem(row + 1, 8), lax.rem(row + 7, 8)
    right, left = lax.rem(col + 1, 8), lax.rem(col + 7, 8)
    cross_down = lax.rem(mp + lax.div(lax.rem(row, 4), 3), 2)
    cross_up = lax.rem(mp + lax.div(lax.rem(row + 3, 4), 3), 2)
    partner = (row, col, 1 - mp)
    straight = [(down, col, mp), (row, right, mp), (up, col, mp), (row, left, mp)]
    crossed = [(down, col, cross_down), (row, right, mp), (up, col, cross_up), (row, left, mp)]

    barrier = pltpu.get_barrier_semaphore()
    for device in [partner] + straight + [crossed[0], crossed[2]]:
        pl.semaphore_signal(barrier, inc=1, device_id=device, device_id_type=MESH)

    def warm_load(e):
        return pltpu.make_async_copy([wd_hbm, wr_hbm][e].at[0, 0], warm.at[e], warm_sem.at[e])

    def w_load(l):
        return pltpu.make_async_copy(w_hbm.at[0, 0, l], w.at[l], w_sem.at[l])

    for e in range(2):
        warm_load(e).start()
    for l in range(2):
        w_load(l).start()

    def warm_copy(e):
        return pltpu.make_async_remote_copy(
            warm.at[e], warm.at[e + 2], warm_send.at[e], warm_recv.at[e], device_id=straight[e], device_id_type=MESH)

    def mp_copy(r, l, e, n):
        return pltpu.make_async_remote_copy(
            send1.at[r, l, pl.ds(e, n)], recv1.at[r, l, pl.ds(e, n)], s1.at[r, l, e // 2], r1.at[r, l, e // 2],
            device_id=partner, device_id_type=MESH)

    def sum_copy(r, l, e):
        return pltpu.make_async_remote_copy(
            send2.at[r, l, e], recv2.at[r, l, (e + 2) % 4], s2.at[r, l], r2.at[r, l],
            device_id=crossed[e], device_id_type=MESH)

    def sums_copy(r, l):
        return pltpu.make_async_remote_copy(
            send2.at[r, l], recv2.at[r, l], s2.at[r, l], r2.at[r, l], device_id=partner, device_id_type=MESH)

    def back_copy(r, l, e):
        return pltpu.make_async_remote_copy(
            send3.at[r, l, e], recv3.at[r, l, (e + 2) % 4], s3.at[r, l], r3.at[r, l],
            device_id=straight[e], device_id_type=MESH)

    def backs_copy(r, l):
        return pltpu.make_async_remote_copy(
            send3.at[r, l], recv3.at[r, l], s3.at[r, l], r3.at[r, l], device_id=partner, device_id_type=MESH)

    def forward(factors, l, turned=True):
        if turned:
            first = dot(factors, wt[l, :, :half], NN)
            second = dot(factors, wt[l, :, half:], NN)
        else:
            first = dot(factors, w[l, :half], NT)
            second = dot(factors, w[l, half:], NT)
        return jnp.where(low_half(first.shape), first, second)

    def first_forward(l, e):
        pieces = []
        for i in (e, e + 1):
            rows = warm[i, l].astype(F32)
            pieces += [rows, rows]
        product = forward(jnp.concatenate(pieces, axis=0).astype(BF16), l, False)
        product = product.reshape(2, 8, half)
        total[l, e:e + 2] = product
        send1[0, l, e:e + 2] = product.astype(BF16)
        mp_copy(0, l, e, 2).start()

    def own_edges(l, _):
        w_load(l).wait()

        @pl.when(l + 2 < layers)
        def _():
            w_load(l + 2).start()

        first_forward(l, 0)

    def other_edges(l, _):
        first_forward(l, 2)

    def add_up(r, l, e, n):
        mp_copy(r, l, e, n).wait_recv()
        value = total[l, e:e + n] + recv1[r, l, e:e + n].astype(F32)
        total[l, e:e + n] = value
        send2[r, l, e:e + n] = value.astype(BF16)
        for i in range(e, e + n):
            sum_copy(r, l, i).start()

    def backward(r, l):
        sums_copy(r, l).wait_recv()

        def mine(j):
            return total[l, :, :, 128 * j:128 * (j + 1)]

        def theirs(j):
            return recv2[r, l, :, :, 128 * j:128 * (j + 1)].astype(F32)

        for j, piece in enumerate(orthonormal(mine, theirs, chunks)):
            p_ref[l, 32 * r:32 * (r + 1), 128 * j:128 * (j + 1)] = piece.reshape(32, 128).astype(BF16)
        basis = p_ref[l, 32 * r:32 * (r + 1)]
        first = dot(basis, w[l, :half], NN)
        second = dot(basis, w[l, half:], NN)
        parts = jnp.where(low_half(first.shape), first, second)
        if r:
            overlap = dot(basis, p_ref[l, :32], NT)
            same = low_half(overlap.shape) == (lax.broadcasted_iota(jnp.int32, overlap.shape, 1) % 8 < 4)
            overlap = jnp.where(same, overlap, 0.0).astype(BF16)
            parts = parts - STEP * dot(overlap, f_ref[l, :32], NN)
        parts = parts.reshape(4, 8, width)
        value = parts + pltpu.roll(parts, 4, 1)
        back[l] = value
        send3[r, l] = value.astype(BF16)
        for e in range(4):
            back_copy(r, l, e).start()

    def combine(r, l):
        backs_copy(r, l).wait_recv()
        value = back[l] + recv3[r, l].astype(F32)
        factors = value.reshape(32, width).astype(BF16)
        f_ref[l, 32 * r:32 * (r + 1)] = factors
        return value, factors

    def second_forward(l, _):
        _, factors = combine(0, l)
        product = forward(factors, l, False)
        overlap = dot(factors, factors, NT)
        same = low_half(overlap.shape) == (lax.broadcasted_iota(jnp.int32, overlap.shape, 1) % 8 < 4)
        overlap = jnp.where(same, overlap, 0.0).astype(BF16)
        product = product - STEP * dot(overlap, p_ref[l, :32], NN)
        product = product.reshape(4, 8, half)
        total[l] = product
        send1[1, l] = product.astype(BF16)
        mp_copy(1, l, 0, 4).start()

    def last(l, _):
        value, _ = combine(1, l)
        cd_ref[l] = value[0, :4]
        cr_ref[l] = value[1, :4]

    def update(l):
        for h in range(2):
            rows = pl.ds(half * h, half)
            w[l, rows] = updated(w[l, rows], p_ref[l], f_ref[l], h)

    def turn(l):
        for j in range(depth // 256):
            wt[l, :, 256 * j:256 * (j + 1)] = w[l, 256 * j:256 * (j + 1)].T

    def each(function, count=layers):
        lax.fori_loop(0, count, lambda l, carry: (function(l, None), carry)[1], 0)

    for e in range(2):
        warm_load(e).wait()
    pl.semaphore_wait(barrier, 7)
    for e in range(2):
        warm_copy(e).start()
    each(own_edges)

    for e in range(2):
        warm_copy(e).wait_recv()
    each(other_edges)
    each(lambda l, _: (add_up(0, l, 0, 2), add_up(0, l, 2, 2)))
    each(lambda l, _: backward(0, l))
    each(second_forward)
    each(lambda l, _: add_up(1, l, 0, 4))
    each(lambda l, _: backward(1, l))
    each(lambda l, _: (last(l, None), update(l)), layers - 1)
    last(layers - 1, None)
    for e in range(2):
        warm_copy(e).wait_send()

    def drain(l, _):
        mp_copy(0, l, 0, 2).wait_send()
        mp_copy(0, l, 2, 2).wait_send()
        mp_copy(1, l, 0, 4).wait_send()
        for r in range(2):
            sums_copy(r, l).wait_send()
            backs_copy(r, l).wait_send()

    each(drain)


def exchange(weights, warm_down, warm_right):
    layers, depth, width = weights.shape[2:]
    half = depth // 2
    vmem = pl.BlockSpec(memory_space=pltpu.VMEM)
    hbm = pl.BlockSpec(memory_space=pltpu.HBM)
    dma = pltpu.SemaphoreType.DMA
    return pl.pallas_call(
        exchange_kernel,
        out_shape=(
            jax.ShapeDtypeStruct((layers, depth, width), BF16),
            jax.ShapeDtypeStruct((layers, 64, half), BF16),
            jax.ShapeDtypeStruct((layers, 64, width), BF16),
            jax.ShapeDtypeStruct((layers, 4, width), F32),
            jax.ShapeDtypeStruct((layers, 4, width), F32),
        ),
        in_specs=[hbm] * 3,
        out_specs=(vmem,) * 5,
        scratch_shapes=[
            pltpu.VMEM((layers, width, depth), BF16),
            pltpu.VMEM((4, layers, 4, width), BF16),
            pltpu.VMEM((layers, 4, 8, half), F32),
            pltpu.VMEM((2, layers, 4, 8, half), BF16),
            pltpu.VMEM((2, layers, 4, 8, half), BF16),
            pltpu.VMEM((2, layers, 4, 8, half), BF16),
            pltpu.VMEM((2, layers, 4, 8, half), BF16),
            pltpu.VMEM((layers, 4, 8, width), F32),
            pltpu.VMEM((2, layers, 4, 8, width), BF16),
            pltpu.VMEM((2, layers, 4, 8, width), BF16),
            dma((layers,)), dma((2,)), dma((2,)), dma((2,)),
            dma((2, layers, 2)), dma((2, layers, 2)),
            dma((2, layers)), dma((2, layers)), dma((2, layers)), dma((2, layers)),
        ],
        compiler_params=pltpu.CompilerParams(collective_id=0, has_side_effects=True, vmem_limit_bytes=36 * 2**20),
        name="exchange",
    )(weights, warm_down, warm_right)


def write_kernel(w_ref, p_ref, f_ref, down_ref, right_ref, w_out, down_out, right_out, rest, sems):
    layers, depth, _ = w_ref.shape
    half, l = depth // 2, layers - 1
    copies = [pltpu.make_async_copy(w_ref.at[i], w_out.at[0, 0, i], sems.at[i]) for i in range(l)]
    copies += [
        pltpu.make_async_copy(down_ref, down_out.at[0, 0], sems.at[l + 2]),
        pltpu.make_async_copy(right_ref, right_out.at[0, 0], sems.at[l + 3]),
    ]
    for copy in copies:
        copy.start()
    for h in range(2):
        rows = pl.ds(half * h, half)
        rest[rows] = updated(w_ref[l, rows], p_ref[l], f_ref[l], h)
        copies.append(pltpu.make_async_copy(rest.at[rows], w_out.at[0, 0, l, rows], sems.at[l + h]))
        copies[-1].start()
    for copy in copies:
        copy.wait()


def write(w, basis, factors, down, right):
    layers, depth, width = w.shape
    vmem = pl.BlockSpec(memory_space=pltpu.VMEM)
    hbm = pl.BlockSpec(memory_space=pltpu.HBM)
    return pl.pallas_call(
        write_kernel,
        out_shape=(
            jax.ShapeDtypeStruct((1, 1, layers, depth, width), BF16),
            jax.ShapeDtypeStruct((1, 1, layers, 4, width), F32),
            jax.ShapeDtypeStruct((1, 1, layers, 4, width), F32),
        ),
        in_specs=[vmem] * 5,
        out_specs=(hbm,) * 3,
        scratch_shapes=[pltpu.VMEM((depth, width), BF16), pltpu.SemaphoreType.DMA((layers + 3,))],
        compiler_params=pltpu.CompilerParams(vmem_limit_bytes=8 * 2**20),
        name="write",
    )(w, basis, factors, down, right)


def body(weights, warm_down, warm_right):
    held = [pltpu.with_memory_space_constraint(x, pltpu.HBM) for x in (weights, warm_down, warm_right)]
    return write(*exchange(*held))


def solution(mesh):
    placed = (P("row", "col", None, None, "mp"),) * 3
    return jax.shard_map(body, mesh=mesh, in_specs=placed, out_specs=placed, check_vma=False)
```

```python
import functools

import jax
import jax.numpy as jnp
from jax import lax
from jax.experimental import pallas as pl
from jax.experimental.pallas import tpu as pltpu
from jax.sharding import PartitionSpec as P

STEP = 0.2
EPS = 1e-06
MESH = pl.DeviceIdType.MESH
F32, BF16 = jnp.float32, jnp.bfloat16
NT = (((1,), (1,)), ((), ()))
NN = (((1,), (0,)), ((), ()))
TN = (((0,), (0,)), ((), ()))


def low_half(shape):
    return lax.broadcasted_iota(jnp.int32, shape, len(shape) - 2) % 8 < 4


def dot(a, b, dims):
    return lax.dot_general(a, b, dims, preferred_element_type=F32)


def orthonormal(total, others, chunks):
    sums = [None] * 4
    for j in range(chunks):
        v = total(j) - others(j)
        for s in range(4):
            term = v * (pltpu.roll(v, s, 1) if s else v)
            sums[s] = term if sums[s] is None else sums[s] + term
    gram = []
    for s in range(4):
        g = jnp.broadcast_to(jnp.sum(sums[s], axis=-1, keepdims=True), sums[s].shape)
        gram.append(g + pltpu.roll(g, 4, 1))

    def at(i, j):
        g = gram[i - j]
        return pltpu.roll(g, 8 - i, 1) if i else g

    g = [[at(i, j) for j in range(i + 1)] for i in range(4)]
    c = [[lax.rsqrt(g[0][0] + EPS)]]
    for k in range(1, 4):
        along = [sum(c[j][i] * g[k][i] for i in range(j + 1)) for j in range(k)]
        m = [-sum(along[j] * c[j][i] for j in range(i, k)) for i in range(k)]
        square = g[k][k]
        for i in range(k):
            inner = 2.0 * g[k][i] + m[i] * g[i][i]
            for j in range(i):
                inner = inner + 2.0 * (m[j] * g[i][j])
            square = square + m[i] * inner
        norm = lax.rsqrt(jnp.maximum(square, 0.0) + EPS)
        c.append([norm * x for x in m] + [norm])
    row = lax.broadcasted_iota(jnp.int32, g[0][0].shape, 1) % 4
    columns = []
    for s in range(4):
        column = jnp.zeros(g[0][0].shape, F32)
        for k in range(s, 4):
            value = c[k][k - s]
            column = jnp.where(row == k, pltpu.roll(value, k, 1) if k else value, column)
        columns.append(column)
    out = []
    for j in range(chunks):
        v = total(j) - others(j)
        p = columns[0] * v
        for s in range(1, 4):
            p = p + columns[s] * pltpu.roll(v, s, 1)
        out.append(p)
    return out


def updated(w, basis, factors, h):
    low = low_half(factors.shape)
    kept = jnp.where(low == (h == 0), factors, jnp.zeros_like(factors))
    return (w.astype(F32) - STEP * dot(basis, kept, TN)).astype(BF16)


def exchange_kernel(
    w_hbm, wd_hbm, wr_hbm, w, p_ref, f_ref, cd_ref, cr_ref,
    wt, warm, total, send1, recv1, send2, recv2, back, send3, recv3,
    w_sem, warm_sem, warm_send, warm_recv, s1, r1, s2, r2, s3, r3,
):
    layers, depth, width = w.shape
    half = depth // 2
    chunks = half // 128
    row, col, mp = lax.axis_index("row"), lax.axis_index("col"), lax.axis_index("mp")
    down, up = lax.rem(row + 1, 8), lax.rem(row + 7, 8)
    right, left = lax.rem(col + 1, 8), lax.rem(col + 7, 8)
    cross_down = lax.rem(mp + lax.div(lax.rem(row, 4), 3), 2)
    cross_up = lax.rem(mp + lax.div(lax.rem(row + 3, 4), 3), 2)
    partner = (row, col, 1 - mp)
    straight = [(down, col, mp), (row, right, mp), (up, col, mp), (row, left, mp)]
    crossed = [(down, col, cross_down), (row, right, mp), (up, col, cross_up), (row, left, mp)]

    barrier = pltpu.get_barrier_semaphore()
    for device in [partner] + straight + [crossed[0], crossed[2]]:
        pl.semaphore_signal(barrier, inc=1, device_id=device, device_id_type=MESH)

    def warm_load(e):
        return pltpu.make_async_copy([wd_hbm, wr_hbm][e].at[0, 0], warm.at[e], warm_sem.at[e])

    def w_load(l):
        return pltpu.make_async_copy(w_hbm.at[0, 0, l], w.at[l], w_sem.at[l])

    for e in range(2):
        warm_load(e).start()
    for l in range(2):
        w_load(l).start()

    def warm_copy(e):
        return pltpu.make_async_remote_copy(
            warm.at[e], warm.at[e + 2], warm_send.at[e], warm_recv.at[e], device_id=straight[e], device_id_type=MESH)

    def mp_copy(r, l, e, n):
        return pltpu.make_async_remote_copy(
            send1.at[r, l, pl.ds(e, n)], recv1.at[r, l, pl.ds(e, n)], s1.at[r, l, e // 2], r1.at[r, l, e // 2],
            device_id=partner, device_id_type=MESH)

    def sum_copy(r, l, e):
        return pltpu.make_async_remote_copy(
            send2.at[r, l, e], recv2.at[r, l, (e + 2) % 4], s2.at[r, l], r2.at[r, l],
            device_id=crossed[e], device_id_type=MESH)

    def sums_copy(r, l):
        return pltpu.make_async_remote_copy(
            send2.at[r, l], recv2.at[r, l], s2.at[r, l], r2.at[r, l], device_id=partner, device_id_type=MESH)

    def back_copy(r, l, e):
        return pltpu.make_async_remote_copy(
            send3.at[r, l, e], recv3.at[r, l, (e + 2) % 4], s3.at[r, l], r3.at[r, l],
            device_id=straight[e], device_id_type=MESH)

    def backs_copy(r, l):
        return pltpu.make_async_remote_copy(
            send3.at[r, l], recv3.at[r, l], s3.at[r, l], r3.at[r, l], device_id=partner, device_id_type=MESH)

    def forward(factors, l, turned):
        first = dot(factors, wt[l, :, :half], NN) if turned else dot(factors, w[l, :half], NT)
        second = dot(factors, wt[l, :, half:], NN) if turned else dot(factors, w[l, half:], NT)
        return jnp.where(low_half(first.shape), first, second)

    def masked(overlap):
        same = low_half(overlap.shape) == (lax.broadcasted_iota(jnp.int32, overlap.shape, 1) % 8 < 4)
        return jnp.where(same, overlap, 0.0).astype(BF16)

    def first_forward(l, e):
        pieces = []
        for i in (e, e + 1):
            rows = warm[i, l].astype(F32)
            pieces += [rows, rows]
        product = forward(jnp.concatenate(pieces, axis=0).astype(BF16), l, e > 0)
        product = product.reshape(2, 8, half)
        total[l, e:e + 2] = product
        send1[0, l, e:e + 2] = product.astype(BF16)
        mp_copy(0, l, e, 2).start()

    def own_edges(l, _):
        w_load(l).wait()

        @pl.when(l + 2 < layers)
        def _():
            w_load(l + 2).start()

        for j in range(depth // 256):
            wt[l, :, 256 * j:256 * (j + 1)] = w[l, 256 * j:256 * (j + 1)].T
        first_forward(l, 0)

    def other_edges(l, _):
        first_forward(l, 2)

    def add_up(r, l, e, n):
        mp_copy(r, l, e, n).wait_recv()
        value = total[l, e:e + n] + recv1[r, l, e:e + n].astype(F32)
        total[l, e:e + n] = value
        send2[r, l, e:e + n] = value.astype(BF16)
        for i in range(e, e + n):
            sum_copy(r, l, i).start()

    def backward(r, l):
        sums_copy(r, l).wait_recv()

        def mine(j):
            return total[l, :, :, 128 * j:128 * (j + 1)]

        def theirs(j):
            return recv2[r, l, :, :, 128 * j:128 * (j + 1)].astype(F32)

        for j, piece in enumerate(orthonormal(mine, theirs, chunks)):
            p_ref[l, 32 * r:32 * (r + 1), 128 * j:128 * (j + 1)] = piece.reshape(32, 128).astype(BF16)
        basis = p_ref[l, 32 * r:32 * (r + 1)]
        if r:
            overlap = masked(dot(basis, p_ref[l, :32], NT))
        first = dot(basis, w[l, :half], NN)
        if r:
            correction = STEP * dot(overlap, f_ref[l, :32], NN)
        second = dot(basis, w[l, half:], NN)
        parts = jnp.where(low_half(first.shape), first, second)
        if r:
            parts = parts - correction
        parts = parts.reshape(4, 8, width)
        value = parts + pltpu.roll(parts, 4, 1)
        back[l] = value
        send3[r, l] = value.astype(BF16)
        for e in range(4):
            back_copy(r, l, e).start()

    def combine(r, l):
        backs_copy(r, l).wait_recv()
        value = back[l] + recv3[r, l].astype(F32)
        factors = value.reshape(32, width).astype(BF16)
        f_ref[l, 32 * r:32 * (r + 1)] = factors
        return value, factors

    def second_forward(l, _):
        _, factors = combine(0, l)
        overlap = masked(dot(factors, factors, NT))
        first = dot(factors, wt[l, :, :half], NN)
        correction = STEP * dot(overlap, p_ref[l, :32], NN)
        second = dot(factors, wt[l, :, half:], NN)
        product = jnp.where(low_half(first.shape), first, second) - correction
        product = product.reshape(4, 8, half)
        total[l] = product
        send1[1, l] = product.astype(BF16)
        mp_copy(1, l, 0, 4).start()

    def last(l, _):
        value, _ = combine(1, l)
        cd_ref[l] = value[0, :4]
        cr_ref[l] = value[1, :4]

    def update(l):
        for h in range(2):
            rows = pl.ds(half * h, half)
            w[l, rows] = updated(w[l, rows], p_ref[l], f_ref[l], h)

    def each(function, count=layers):
        lax.fori_loop(0, count, lambda l, carry: (function(l, None), carry)[1], 0)

    for e in range(2):
        warm_load(e).wait()
    pl.semaphore_wait(barrier, 7)
    for e in range(2):
        warm_copy(e).start()
    each(own_edges)

    for e in range(2):
        warm_copy(e).wait_recv()
    each(other_edges)
    each(lambda l, _: (add_up(0, l, 0, 2), add_up(0, l, 2, 2)))
    each(lambda l, _: backward(0, l))
    each(second_forward)
    each(lambda l, _: add_up(1, l, 0, 4))
    each(lambda l, _: backward(1, l))
    for e in range(2):
        warm_copy(e).wait_send()

    def drain(l, _):
        mp_copy(0, l, 0, 2).wait_send()
        mp_copy(0, l, 2, 2).wait_send()
        mp_copy(1, l, 0, 4).wait_send()
        sums_copy(0, l).wait_send()
        sums_copy(1, l).wait_send()
        backs_copy(0, l).wait_send()

    each(drain)

    def finish(l, _):
        last(l, None)
        update(l)
        backs_copy(1, l).wait_send()

    each(finish, layers - 1)
    last(layers - 1, None)
    backs_copy(1, layers - 1).wait_send()


def exchange(weights, warm_down, warm_right):
    layers, depth, width = weights.shape[2:]
    half = depth // 2
    vmem = pl.BlockSpec(memory_space=pltpu.VMEM)
    hbm = pl.BlockSpec(memory_space=pltpu.HBM)
    dma = pltpu.SemaphoreType.DMA
    return pl.pallas_call(
        exchange_kernel,
        out_shape=(
            jax.ShapeDtypeStruct((layers, depth, width), BF16),
            jax.ShapeDtypeStruct((layers, 64, half), BF16),
            jax.ShapeDtypeStruct((layers, 64, width), BF16),
            jax.ShapeDtypeStruct((layers, 4, width), F32),
            jax.ShapeDtypeStruct((layers, 4, width), F32),
        ),
        in_specs=[hbm] * 3,
        out_specs=(vmem,) * 5,
        scratch_shapes=[
            pltpu.VMEM((layers, width, depth), BF16),
            pltpu.VMEM((4, layers, 4, width), BF16),
            pltpu.VMEM((layers, 4, 8, half), F32),
            pltpu.VMEM((2, layers, 4, 8, half), BF16),
            pltpu.VMEM((2, layers, 4, 8, half), BF16),
            pltpu.VMEM((2, layers, 4, 8, half), BF16),
            pltpu.VMEM((2, layers, 4, 8, half), BF16),
            pltpu.VMEM((layers, 4, 8, width), F32),
            pltpu.VMEM((2, layers, 4, 8, width), BF16),
            pltpu.VMEM((2, layers, 4, 8, width), BF16),
            dma((layers,)), dma((2,)), dma((2,)), dma((2,)),
            dma((2, layers, 2)), dma((2, layers, 2)),
            dma((2, layers)), dma((2, layers)), dma((2, layers)), dma((2, layers)),
        ],
        compiler_params=pltpu.CompilerParams(collective_id=0, has_side_effects=True, vmem_limit_bytes=36 * 2**20),
        name="exchange",
    )(weights, warm_down, warm_right)


def write_kernel(w_ref, p_ref, f_ref, down_ref, right_ref, w_out, down_out, right_out, rest, sems):
    layers, depth, _ = w_ref.shape
    half, l = depth // 2, layers - 1
    copies = [
        pltpu.make_async_copy(down_ref, down_out.at[0, 0], sems.at[l, 0]),
        pltpu.make_async_copy(right_ref, right_out.at[0, 0], sems.at[l, 1]),
    ]
    for i in range(l):
        for h in range(2):
            rows = pl.ds(half * h, half)
            copies.append(pltpu.make_async_copy(w_ref.at[i, rows], w_out.at[0, 0, i, rows], sems.at[i, h]))
    for copy in copies:
        copy.start()
    for h in range(2):
        rows = pl.ds(half * h, half)
        rest[rows] = updated(w_ref[l, rows], p_ref[l], f_ref[l], h)
        copies.append(pltpu.make_async_copy(rest.at[rows], w_out.at[0, 0, l, rows], sems.at[l + 1, h]))
        copies[-1].start()
    for copy in copies:
        copy.wait()


def write(w, basis, factors, down, right):
    layers, depth, width = w.shape
    vmem = pl.BlockSpec(memory_space=pltpu.VMEM)
    hbm = pl.BlockSpec(memory_space=pltpu.HBM)
    return pl.pallas_call(
        write_kernel,
        out_shape=(
            jax.ShapeDtypeStruct((1, 1, layers, depth, width), BF16),
            jax.ShapeDtypeStruct((1, 1, layers, 4, width), F32),
            jax.ShapeDtypeStruct((1, 1, layers, 4, width), F32),
        ),
        in_specs=[vmem] * 5,
        out_specs=(hbm,) * 3,
        scratch_shapes=[pltpu.VMEM((depth, width), BF16), pltpu.SemaphoreType.DMA((layers + 1, 2))],
        compiler_params=pltpu.CompilerParams(vmem_limit_bytes=8 * 2**20),
        name="write",
    )(w, basis, factors, down, right)


def body(weights, warm_down, warm_right):
    held = [pltpu.with_memory_space_constraint(x, pltpu.HBM) for x in (weights, warm_down, warm_right)]
    return write(*exchange(*held))


def solution(mesh):
    placed = (P("row", "col", None, None, "mp"),) * 3
    return jax.shard_map(body, mesh=mesh, in_specs=placed, out_specs=placed, check_vma=False)
```

```python
import functools

import jax
import jax.numpy as jnp
from jax import lax
from jax.experimental import pallas as pl
from jax.experimental.pallas import tpu as pltpu
from jax.sharding import PartitionSpec as P

STEP = 0.2
EPS = 1e-06
MESH = pl.DeviceIdType.MESH
F32, BF16 = jnp.float32, jnp.bfloat16
NT = (((1,), (1,)), ((), ()))
NN = (((1,), (0,)), ((), ()))
TN = (((0,), (0,)), ((), ()))


def low_half(shape):
    return lax.broadcasted_iota(jnp.int32, shape, len(shape) - 2) % 8 < 4


def dot(a, b, dims):
    return lax.dot_general(a, b, dims, preferred_element_type=F32)


def orthonormal(total, others, chunks):
    sums = [None] * 4
    for j in range(chunks):
        v = total(j) - others(j)
        for s in range(4):
            term = v * (pltpu.roll(v, s, 1) if s else v)
            sums[s] = term if sums[s] is None else sums[s] + term
    gram = []
    for s in range(4):
        g = jnp.broadcast_to(jnp.sum(sums[s], axis=-1, keepdims=True), sums[s].shape)
        gram.append(g + pltpu.roll(g, 4, 1))

    def at(i, j):
        g = gram[i - j]
        return pltpu.roll(g, 8 - i, 1) if i else g

    g = [[at(i, j) for j in range(i + 1)] for i in range(4)]
    c = [[lax.rsqrt(g[0][0] + EPS)]]
    for k in range(1, 4):
        along = [sum(c[j][i] * g[k][i] for i in range(j + 1)) for j in range(k)]
        m = [-sum(along[j] * c[j][i] for j in range(i, k)) for i in range(k)]
        square = g[k][k]
        for i in range(k):
            inner = 2.0 * g[k][i] + m[i] * g[i][i]
            for j in range(i):
                inner = inner + 2.0 * (m[j] * g[i][j])
            square = square + m[i] * inner
        norm = lax.rsqrt(jnp.maximum(square, 0.0) + EPS)
        c.append([norm * x for x in m] + [norm])
    row = lax.broadcasted_iota(jnp.int32, g[0][0].shape, 1) % 4
    columns = []
    for s in range(4):
        column = jnp.zeros(g[0][0].shape, F32)
        for k in range(s, 4):
            value = c[k][k - s]
            column = jnp.where(row == k, pltpu.roll(value, k, 1) if k else value, column)
        columns.append(column)
    out = []
    for j in range(chunks):
        v = total(j) - others(j)
        p = columns[0] * v
        for s in range(1, 4):
            p = p + columns[s] * pltpu.roll(v, s, 1)
        out.append(p)
    return out


def updated(w, basis, factors, h):
    low = low_half(factors.shape)
    kept = jnp.where(low == (h == 0), factors, jnp.zeros_like(factors))
    return (w.astype(F32) - STEP * dot(basis, kept, TN)).astype(BF16)


def exchange_kernel(
    w_hbm, wd_hbm, wr_hbm, w, p_ref, f_ref, cd_ref, cr_ref,
    wt, warm, total, send1, recv1, send2, recv2, back, send3, recv3,
    w_sem, warm_sem, warm_send, warm_recv, s1, r1, s2, r2, s3, r3,
):
    layers, depth, width = w.shape
    half = depth // 2
    chunks = half // 128
    row, col, mp = lax.axis_index("row"), lax.axis_index("col"), lax.axis_index("mp")
    down, up = lax.rem(row + 1, 8), lax.rem(row + 7, 8)
    right, left = lax.rem(col + 1, 8), lax.rem(col + 7, 8)
    cross_down = lax.rem(mp + lax.div(lax.rem(row, 4), 3), 2)
    cross_up = lax.rem(mp + lax.div(lax.rem(row + 3, 4), 3), 2)
    partner = (row, col, 1 - mp)
    straight = [(down, col, mp), (row, right, mp), (up, col, mp), (row, left, mp)]
    crossed = [(down, col, cross_down), (row, right, mp), (up, col, cross_up), (row, left, mp)]

    barrier = pltpu.get_barrier_semaphore()
    for device in [partner] + straight + [crossed[0], crossed[2]]:
        pl.semaphore_signal(barrier, inc=1, device_id=device, device_id_type=MESH)

    def warm_load(e):
        return pltpu.make_async_copy([wd_hbm, wr_hbm][e].at[0, 0], warm.at[e], warm_sem.at[e])

    def w_load(l):
        return pltpu.make_async_copy(w_hbm.at[0, 0, l], w.at[l], w_sem.at[l])

    for e in range(2):
        warm_load(e).start()
    for l in range(3):
        w_load(l).start()

    def warm_copy(e):
        return pltpu.make_async_remote_copy(
            warm.at[e], warm.at[e + 2], warm_send.at[e], warm_recv.at[e], device_id=straight[e], device_id_type=MESH)

    def mp_copy(r, l, e):
        return pltpu.make_async_remote_copy(
            send1.at[r, l, e], recv1.at[r, l, e], s1.at[r, l, e], r1.at[r, l, e],
            device_id=partner, device_id_type=MESH)

    def sum_copy(r, l, e):
        return pltpu.make_async_remote_copy(
            send2.at[r, l, e], recv2.at[r, l, (e + 2) % 4], s2.at[r, l], r2.at[r, l],
            device_id=crossed[e], device_id_type=MESH)

    def sums_copy(r, l):
        return pltpu.make_async_remote_copy(
            send2.at[r, l], recv2.at[r, l], s2.at[r, l], r2.at[r, l], device_id=partner, device_id_type=MESH)

    def back_copy(r, l, e):
        return pltpu.make_async_remote_copy(
            send3.at[r, l, e], recv3.at[r, l, (e + 2) % 4], s3.at[r, l], r3.at[r, l],
            device_id=straight[e], device_id_type=MESH)

    def backs_copy(r, l):
        return pltpu.make_async_remote_copy(
            send3.at[r, l], recv3.at[r, l], s3.at[r, l], r3.at[r, l], device_id=partner, device_id_type=MESH)

    def forward(factors, l, turned):
        first = dot(factors, wt[l, :, :half], NN) if turned else dot(factors, w[l, :half], NT)
        second = dot(factors, wt[l, :, half:], NN) if turned else dot(factors, w[l, half:], NT)
        return jnp.where(low_half(first.shape), first, second)

    def masked(overlap):
        same = low_half(overlap.shape) == (lax.broadcasted_iota(jnp.int32, overlap.shape, 1) % 8 < 4)
        return jnp.where(same, overlap, 0.0).astype(BF16)

    def first_forward(l, e):
        pieces = []
        for i in (e, e + 1):
            rows = warm[i, l].astype(F32)
            pieces += [rows, rows]
        product = forward(jnp.concatenate(pieces, axis=0).astype(BF16), l, e > 0)
        product = product.reshape(2, 8, half)
        total[l, e:e + 2] = product
        send1[0, l, e:e + 2] = product.astype(BF16)
        for i in (e, e + 1):
            mp_copy(0, l, i).start()

    def own_edges(l, _):
        w_load(l).wait()

        @pl.when(l + 3 < layers)
        def _():
            w_load(l + 3).start()

        for j in range(depth // 256):
            wt[l, :, 256 * j:256 * (j + 1)] = w[l, 256 * j:256 * (j + 1)].T
        first_forward(l, 0)

    def other_edges(l, _):
        first_forward(l, 2)

    def add_up(r, l, slots):
        for e in slots:
            mp_copy(r, l, e).wait_recv()
            value = total[l, e] + recv1[r, l, e].astype(F32)
            total[l, e] = value
            send2[r, l, e] = value.astype(BF16)
            sum_copy(r, l, e).start()

    def backward(r, l):
        sums_copy(r, l).wait_recv()

        def mine(j):
            return total[l, :, :, 128 * j:128 * (j + 1)]

        def theirs(j):
            return recv2[r, l, :, :, 128 * j:128 * (j + 1)].astype(F32)

        for j, piece in enumerate(orthonormal(mine, theirs, chunks)):
            p_ref[l, 32 * r:32 * (r + 1), 128 * j:128 * (j + 1)] = piece.reshape(32, 128).astype(BF16)
        basis = p_ref[l, 32 * r:32 * (r + 1)]
        if r:
            overlap = masked(dot(basis, p_ref[l, :32], NT))
        first = dot(basis, w[l, :half], NN)
        if r:
            correction = STEP * dot(overlap, f_ref[l, :32], NN)
        second = dot(basis, w[l, half:], NN)
        parts = jnp.where(low_half(first.shape), first, second)
        if r:
            parts = parts - correction
        parts = parts.reshape(4, 8, width)
        value = parts + pltpu.roll(parts, 4, 1)
        back[l] = value
        send3[r, l] = value.astype(BF16)
        for e in (0, 2, 1, 3):
            back_copy(r, l, e).start()

    def combine(r, l):
        backs_copy(r, l).wait_recv()
        value = back[l] + recv3[r, l].astype(F32)
        factors = value.reshape(32, width).astype(BF16)
        f_ref[l, 32 * r:32 * (r + 1)] = factors
        return value, factors

    def second_forward(l, _):
        _, factors = combine(0, l)
        overlap = masked(dot(factors, factors, NT))
        first = dot(factors, wt[l, :, :half], NN)
        correction = STEP * dot(overlap, p_ref[l, :32], NN)
        second = dot(factors, wt[l, :, half:], NN)
        product = jnp.where(low_half(first.shape), first, second) - correction
        product = product.reshape(4, 8, half)
        total[l] = product
        send1[1, l] = product.astype(BF16)
        for e in (0, 2, 1, 3):
            mp_copy(1, l, e).start()

    def last(l, _):
        value, _ = combine(1, l)
        cd_ref[l] = value[0, :4]
        cr_ref[l] = value[1, :4]

    def update(l):
        for h in range(2):
            rows = pl.ds(half * h, half)
            w[l, rows] = updated(w[l, rows], p_ref[l], f_ref[l], h)

    def each(function, count=layers):
        lax.fori_loop(0, count, lambda l, carry: (function(l, None), carry)[1], 0)

    for e in range(2):
        warm_load(e).wait()
    pl.semaphore_wait(barrier, 7)
    for e in range(2):
        warm_copy(e).start()
    each(own_edges)

    for e in range(2):
        warm_copy(e).wait_recv()
    each(other_edges)
    each(lambda l, _: add_up(0, l, (0, 1, 2, 3)))
    each(lambda l, _: backward(0, l))
    each(second_forward)
    each(lambda l, _: add_up(1, l, (0, 2, 1, 3)))
    each(lambda l, _: backward(1, l))
    for e in range(2):
        warm_copy(e).wait_send()

    def drain(l, _):
        for r in range(2):
            for e in range(4):
                mp_copy(r, l, e).wait_send()
        sums_copy(0, l).wait_send()
        sums_copy(1, l).wait_send()
        backs_copy(0, l).wait_send()

    each(drain)

    def finish(l, _):
        last(l, None)
        update(l)
        backs_copy(1, l).wait_send()

    each(finish, layers - 1)
    last(layers - 1, None)
    backs_copy(1, layers - 1).wait_send()


def exchange(weights, warm_down, warm_right):
    layers, depth, width = weights.shape[2:]
    half = depth // 2
    vmem = pl.BlockSpec(memory_space=pltpu.VMEM)
    hbm = pl.BlockSpec(memory_space=pltpu.HBM)
    dma = pltpu.SemaphoreType.DMA
    return pl.pallas_call(
        exchange_kernel,
        out_shape=(
            jax.ShapeDtypeStruct((layers, depth, width), BF16),
            jax.ShapeDtypeStruct((layers, 64, half), BF16),
            jax.ShapeDtypeStruct((layers, 64, width), BF16),
            jax.ShapeDtypeStruct((layers, 4, width), F32),
            jax.ShapeDtypeStruct((layers, 4, width), F32),
        ),
        in_specs=[hbm] * 3,
        out_specs=(vmem,) * 5,
        scratch_shapes=[
            pltpu.VMEM((layers, width, depth), BF16),
            pltpu.VMEM((4, layers, 4, width), BF16),
            pltpu.VMEM((layers, 4, 8, half), F32),
            pltpu.VMEM((2, layers, 4, 8, half), BF16),
            pltpu.VMEM((2, layers, 4, 8, half), BF16),
            pltpu.VMEM((2, layers, 4, 8, half), BF16),
            pltpu.VMEM((2, layers, 4, 8, half), BF16),
            pltpu.VMEM((layers, 4, 8, width), F32),
            pltpu.VMEM((2, layers, 4, 8, width), BF16),
            pltpu.VMEM((2, layers, 4, 8, width), BF16),
            dma((layers,)), dma((2,)), dma((2,)), dma((2,)),
            dma((2, layers, 4)), dma((2, layers, 4)),
            dma((2, layers)), dma((2, layers)), dma((2, layers)), dma((2, layers)),
        ],
        compiler_params=pltpu.CompilerParams(collective_id=0, has_side_effects=True, vmem_limit_bytes=36 * 2**20),
        name="exchange",
    )(weights, warm_down, warm_right)


def write_kernel(w_ref, p_ref, f_ref, down_ref, right_ref, w_out, down_out, right_out, rest, sems):
    layers, depth, _ = w_ref.shape
    half, l = depth // 2, layers - 1
    copies = [
        pltpu.make_async_copy(down_ref, down_out.at[0, 0], sems.at[l, 0]),
        pltpu.make_async_copy(right_ref, right_out.at[0, 0], sems.at[l, 1]),
    ]
    for i in range(l):
        for h in range(2):
            rows = pl.ds(half * h, half)
            copies.append(pltpu.make_async_copy(w_ref.at[i, rows], w_out.at[0, 0, i, rows], sems.at[i, h]))
    for copy in copies:
        copy.start()
    for h in range(2):
        rows = pl.ds(half * h, half)
        rest[rows] = updated(w_ref[l, rows], p_ref[l], f_ref[l], h)
        copies.append(pltpu.make_async_copy(rest.at[rows], w_out.at[0, 0, l, rows], sems.at[l + 1, h]))
        copies[-1].start()
    for copy in copies:
        copy.wait()


def write(w, basis, factors, down, right):
    layers, depth, width = w.shape
    vmem = pl.BlockSpec(memory_space=pltpu.VMEM)
    hbm = pl.BlockSpec(memory_space=pltpu.HBM)
    return pl.pallas_call(
        write_kernel,
        out_shape=(
            jax.ShapeDtypeStruct((1, 1, layers, depth, width), BF16),
            jax.ShapeDtypeStruct((1, 1, layers, 4, width), F32),
            jax.ShapeDtypeStruct((1, 1, layers, 4, width), F32),
        ),
        in_specs=[vmem] * 5,
        out_specs=(hbm,) * 3,
        scratch_shapes=[pltpu.VMEM((depth, width), BF16), pltpu.SemaphoreType.DMA((layers + 1, 2))],
        compiler_params=pltpu.CompilerParams(vmem_limit_bytes=8 * 2**20),
        name="write",
    )(w, basis, factors, down, right)


def body(weights, warm_down, warm_right):
    held = [pltpu.with_memory_space_constraint(x, pltpu.HBM) for x in (weights, warm_down, warm_right)]
    return write(*exchange(*held))


def solution(mesh):
    placed = (P("row", "col", None, None, "mp"),) * 3
    return jax.shard_map(body, mesh=mesh, in_specs=placed, out_specs=placed, check_vma=False)
```

```python
import functools

import jax
import jax.numpy as jnp
from jax import lax
from jax.experimental import pallas as pl
from jax.experimental.pallas import tpu as pltpu
from jax.sharding import PartitionSpec as P

STEP = 0.2
EPS = 1e-06
MESH = pl.DeviceIdType.MESH
F32, BF16 = jnp.float32, jnp.bfloat16
NT = (((1,), (1,)), ((), ()))
NN = (((1,), (0,)), ((), ()))
TN = (((0,), (0,)), ((), ()))


def low_half(shape):
    return lax.broadcasted_iota(jnp.int32, shape, len(shape) - 2) % 8 < 4


def dot(a, b, dims):
    return lax.dot_general(a, b, dims, preferred_element_type=F32)


def orthonormal(total, others, chunks):
    sums = [None] * 4
    for j in range(chunks):
        v = total(j) - others(j)
        for s in range(4):
            term = v * (pltpu.roll(v, s, 1) if s else v)
            sums[s] = term if sums[s] is None else sums[s] + term
    gram = []
    for s in range(4):
        g = jnp.broadcast_to(jnp.sum(sums[s], axis=-1, keepdims=True), sums[s].shape)
        gram.append(g + pltpu.roll(g, 4, 1))

    def at(i, j):
        g = gram[i - j]
        return pltpu.roll(g, 8 - i, 1) if i else g

    g = [[at(i, j) for j in range(i + 1)] for i in range(4)]
    c = [[lax.rsqrt(g[0][0] + EPS)]]
    for k in range(1, 4):
        along = [sum(c[j][i] * g[k][i] for i in range(j + 1)) for j in range(k)]
        m = [-sum(along[j] * c[j][i] for j in range(i, k)) for i in range(k)]
        square = g[k][k]
        for i in range(k):
            inner = 2.0 * g[k][i] + m[i] * g[i][i]
            for j in range(i):
                inner = inner + 2.0 * (m[j] * g[i][j])
            square = square + m[i] * inner
        norm = lax.rsqrt(jnp.maximum(square, 0.0) + EPS)
        c.append([norm * x for x in m] + [norm])
    row = lax.broadcasted_iota(jnp.int32, g[0][0].shape, 1) % 4
    columns = []
    for s in range(4):
        column = jnp.zeros(g[0][0].shape, F32)
        for k in range(s, 4):
            value = c[k][k - s]
            column = jnp.where(row == k, pltpu.roll(value, k, 1) if k else value, column)
        columns.append(column)
    out = []
    for j in range(chunks):
        v = total(j) - others(j)
        p = columns[0] * v
        for s in range(1, 4):
            p = p + columns[s] * pltpu.roll(v, s, 1)
        out.append(p)
    return out


def updated(w, basis, factors, h):
    low = low_half(factors.shape)
    kept = jnp.where(low == (h == 0), factors, jnp.zeros_like(factors))
    return (w.astype(F32) - STEP * dot(basis, kept, TN)).astype(BF16)


def exchange_kernel(
    w_hbm, wd_hbm, wr_hbm, w, p_ref, f_ref, cd_ref, cr_ref,
    wt, warm, total, send1, recv1, send2, recv2, back, send3, recv3,
    w_sem, warm_sem, warm_send, warm_recv, s1, r1, s2, r2, s3, r3,
):
    layers, depth, width = w.shape
    half = depth // 2
    chunks = half // 128
    row, col, mp = lax.axis_index("row"), lax.axis_index("col"), lax.axis_index("mp")
    down, up = lax.rem(row + 1, 8), lax.rem(row + 7, 8)
    right, left = lax.rem(col + 1, 8), lax.rem(col + 7, 8)
    cross_down = lax.rem(mp + lax.div(lax.rem(row, 4), 3), 2)
    cross_up = lax.rem(mp + lax.div(lax.rem(row + 3, 4), 3), 2)
    partner = (row, col, 1 - mp)
    straight = [(down, col, mp), (row, right, mp), (up, col, mp), (row, left, mp)]
    crossed = [(down, col, cross_down), (row, right, mp), (up, col, cross_up), (row, left, mp)]

    barrier = pltpu.get_barrier_semaphore()
    for device in [partner] + straight + [crossed[0], crossed[2]]:
        pl.semaphore_signal(barrier, inc=1, device_id=device, device_id_type=MESH)

    def warm_load(e):
        return pltpu.make_async_copy([wd_hbm, wr_hbm][e].at[0, 0], warm.at[e], warm_sem.at[e])

    def w_load(l):
        return pltpu.make_async_copy(w_hbm.at[0, 0, l], w.at[l], w_sem.at[l])

    for e in range(2):
        warm_load(e).start()
    for l in range(3):
        w_load(l).start()

    def warm_copy(e):
        return pltpu.make_async_remote_copy(
            warm.at[e], warm.at[e + 2], warm_send.at[e], warm_recv.at[e], device_id=straight[e], device_id_type=MESH)

    def mp_copy(r, l, e):
        return pltpu.make_async_remote_copy(
            send1.at[r, l, e], recv1.at[r, l, e], s1.at[r, l, e], r1.at[r, l, e],
            device_id=partner, device_id_type=MESH)

    def sum_copy(r, l, e):
        return pltpu.make_async_remote_copy(
            send2.at[r, l, e], recv2.at[r, l, (e + 2) % 4], s2.at[r, l], r2.at[r, l],
            device_id=crossed[e], device_id_type=MESH)

    def sums_copy(r, l):
        return pltpu.make_async_remote_copy(
            send2.at[r, l], recv2.at[r, l], s2.at[r, l], r2.at[r, l], device_id=partner, device_id_type=MESH)

    def back_copy(r, l, e):
        return pltpu.make_async_remote_copy(
            send3.at[r, l, e], recv3.at[r, l, (e + 2) % 4], s3.at[r, l], r3.at[r, l],
            device_id=straight[e], device_id_type=MESH)

    def backs_copy(r, l):
        return pltpu.make_async_remote_copy(
            send3.at[r, l], recv3.at[r, l], s3.at[r, l], r3.at[r, l], device_id=partner, device_id_type=MESH)

    def forward(factors, l, turned):
        first = dot(factors, wt[l, :, :half], NN) if turned else dot(factors, w[l, :half], NT)
        second = dot(factors, wt[l, :, half:], NN) if turned else dot(factors, w[l, half:], NT)
        return jnp.where(low_half(first.shape), first, second)

    def masked(overlap):
        same = low_half(overlap.shape) == (lax.broadcasted_iota(jnp.int32, overlap.shape, 1) % 8 < 4)
        return jnp.where(same, overlap, 0.0).astype(BF16)

    def first_forward(l, e):
        pieces = []
        for i in (e, e + 1):
            rows = warm[i, l].astype(F32)
            pieces += [rows, rows]
        product = forward(jnp.concatenate(pieces, axis=0).astype(BF16), l, e > 0)
        product = product.reshape(2, 8, half)
        total[l, e:e + 2] = product
        send1[0, l, e:e + 2] = product.astype(BF16)
        for i in (e, e + 1):
            mp_copy(0, l, i).start()

    def own_edges(l, _):
        w_load(l).wait()

        @pl.when(l + 3 < layers)
        def _():
            w_load(l + 3).start()

        for j in range(depth // 256):
            wt[l, :, 256 * j:256 * (j + 1)] = w[l, 256 * j:256 * (j + 1)].T
        first_forward(l, 0)

    def other_edges(l, _):
        first_forward(l, 2)

    def add_up(r, l, slots):
        for e in slots:
            mp_copy(r, l, e).wait_recv()
            value = total[l, e] + recv1[r, l, e].astype(F32)
            total[l, e] = value
            send2[r, l, e] = value.astype(BF16)
            sum_copy(r, l, e).start()

    def backward(r, l):
        sums_copy(r, l).wait_recv()

        def mine(j):
            return total[l, :, :, 128 * j:128 * (j + 1)]

        def theirs(j):
            return recv2[r, l, :, :, 128 * j:128 * (j + 1)].astype(F32)

        for j, piece in enumerate(orthonormal(mine, theirs, chunks)):
            p_ref[l, 32 * r:32 * (r + 1), 128 * j:128 * (j + 1)] = piece.reshape(32, 128).astype(BF16)
        basis = p_ref[l, 32 * r:32 * (r + 1)]
        if r:
            overlap = masked(dot(basis, p_ref[l, :32], NT))
        first = dot(basis, w[l, :half], NN)
        if r:
            correction = STEP * dot(overlap, f_ref[l, :32], NN)
        second = dot(basis, w[l, half:], NN)
        parts = jnp.where(low_half(first.shape), first, second)
        if r:
            parts = parts - correction
        parts = parts.reshape(4, 8, width)
        value = parts + pltpu.roll(parts, 4, 1)
        back[l] = value
        send3[r, l] = value.astype(BF16)
        for e in (0, 2, 1, 3):
            back_copy(r, l, e).start()

    def combine(r, l):
        backs_copy(r, l).wait_recv()
        value = back[l] + recv3[r, l].astype(F32)
        factors = value.reshape(32, width).astype(BF16)
        f_ref[l, 32 * r:32 * (r + 1)] = factors
        return value, factors

    def second_forward(l, _):
        _, factors = combine(0, l)
        overlap = masked(dot(factors, factors, NT))
        first = dot(factors, wt[l, :, :half], NN)
        correction = STEP * dot(overlap, p_ref[l, :32], NN)
        second = dot(factors, wt[l, :, half:], NN)
        product = jnp.where(low_half(first.shape), first, second) - correction
        product = product.reshape(4, 8, half)
        total[l] = product
        send1[1, l] = product.astype(BF16)
        for e in (0, 2, 1, 3):
            mp_copy(1, l, e).start()

    def last(l, _):
        value, _ = combine(1, l)
        cd_ref[l] = value[0, :4]
        cr_ref[l] = value[1, :4]

    def update(l):
        for h in range(2):
            rows = pl.ds(half * h, half)
            w[l, rows] = updated(w[l, rows], p_ref[l], f_ref[l], h)

    def each(function, count=layers):
        lax.fori_loop(0, count, lambda l, carry: (function(l, None), carry)[1], 0)

    for e in range(2):
        warm_load(e).wait()
    pl.semaphore_wait(barrier, 7)
    for e in range(2):
        warm_copy(e).start()
    each(own_edges)

    for e in range(2):
        warm_copy(e).wait_recv()
    each(other_edges)
    each(lambda l, _: add_up(0, l, (0, 1, 2, 3)))
    each(lambda l, _: backward(0, l))
    each(second_forward)
    each(lambda l, _: add_up(1, l, (0, 2, 1, 3)))
    each(lambda l, _: backward(1, l))
    for e in range(2):
        warm_copy(e).wait_send()

    def drain(l, _):
        for r in range(2):
            for e in range(4):
                mp_copy(r, l, e).wait_send()
        sums_copy(0, l).wait_send()
        sums_copy(1, l).wait_send()
        backs_copy(0, l).wait_send()

    each(drain)

    def finish(l, _):
        last(l, None)
        update(l)
        backs_copy(1, l).wait_send()

    each(finish, layers - 2)
    for l in (layers - 2, layers - 1):
        last(l, None)
        backs_copy(1, l).wait_send()


def exchange(weights, warm_down, warm_right):
    layers, depth, width = weights.shape[2:]
    half = depth // 2
    vmem = pl.BlockSpec(memory_space=pltpu.VMEM)
    hbm = pl.BlockSpec(memory_space=pltpu.HBM)
    dma = pltpu.SemaphoreType.DMA
    return pl.pallas_call(
        exchange_kernel,
        out_shape=(
            jax.ShapeDtypeStruct((layers, depth, width), BF16),
            jax.ShapeDtypeStruct((layers, 64, half), BF16),
            jax.ShapeDtypeStruct((layers, 64, width), BF16),
            jax.ShapeDtypeStruct((layers, 4, width), F32),
            jax.ShapeDtypeStruct((layers, 4, width), F32),
        ),
        in_specs=[hbm] * 3,
        out_specs=(vmem,) * 5,
        scratch_shapes=[
            pltpu.VMEM((layers, width, depth), BF16),
            pltpu.VMEM((4, layers, 4, width), BF16),
            pltpu.VMEM((layers, 4, 8, half), F32),
            pltpu.VMEM((2, layers, 4, 8, half), BF16),
            pltpu.VMEM((2, layers, 4, 8, half), BF16),
            pltpu.VMEM((2, layers, 4, 8, half), BF16),
            pltpu.VMEM((2, layers, 4, 8, half), BF16),
            pltpu.VMEM((layers, 4, 8, width), F32),
            pltpu.VMEM((2, layers, 4, 8, width), BF16),
            pltpu.VMEM((2, layers, 4, 8, width), BF16),
            dma((layers,)), dma((2,)), dma((2,)), dma((2,)),
            dma((2, layers, 4)), dma((2, layers, 4)),
            dma((2, layers)), dma((2, layers)), dma((2, layers)), dma((2, layers)),
        ],
        compiler_params=pltpu.CompilerParams(collective_id=0, has_side_effects=True, vmem_limit_bytes=36 * 2**20),
        name="exchange",
    )(weights, warm_down, warm_right)


def write_kernel(w_ref, p_ref, f_ref, down_ref, right_ref, w_out, down_out, right_out, rest, sems):
    layers, depth, _ = w_ref.shape
    half, kept = depth // 2, layers - 2
    copies = [
        pltpu.make_async_copy(down_ref, down_out.at[0, 0], sems.at[layers, 0]),
        pltpu.make_async_copy(right_ref, right_out.at[0, 0], sems.at[layers, 1]),
    ]
    for l in range(kept):
        for h in range(2):
            rows = pl.ds(half * h, half)
            copies.append(pltpu.make_async_copy(w_ref.at[l, rows], w_out.at[0, 0, l, rows], sems.at[l, h]))
    for copy in copies:
        copy.start()
    for l in range(kept, layers):
        for h in range(2):
            rows = pl.ds(half * h, half)
            rest[l - kept, rows] = updated(w_ref[l, rows], p_ref[l], f_ref[l], h)
            copies.append(pltpu.make_async_copy(rest.at[l - kept, rows], w_out.at[0, 0, l, rows], sems.at[l, h]))
            copies[-1].start()
    for copy in copies:
        copy.wait()


def write(w, basis, factors, down, right):
    layers, depth, width = w.shape
    vmem = pl.BlockSpec(memory_space=pltpu.VMEM)
    hbm = pl.BlockSpec(memory_space=pltpu.HBM)
    return pl.pallas_call(
        write_kernel,
        out_shape=(
            jax.ShapeDtypeStruct((1, 1, layers, depth, width), BF16),
            jax.ShapeDtypeStruct((1, 1, layers, 4, width), F32),
            jax.ShapeDtypeStruct((1, 1, layers, 4, width), F32),
        ),
        in_specs=[vmem] * 5,
        out_specs=(hbm,) * 3,
        scratch_shapes=[pltpu.VMEM((2, depth, width), BF16), pltpu.SemaphoreType.DMA((layers + 1, 2))],
        compiler_params=pltpu.CompilerParams(vmem_limit_bytes=10 * 2**20),
        name="write",
    )(w, basis, factors, down, right)


def body(weights, warm_down, warm_right):
    held = [pltpu.with_memory_space_constraint(x, pltpu.HBM) for x in (weights, warm_down, warm_right)]
    return write(*exchange(*held))


def solution(mesh):
    placed = (P("row", "col", None, None, "mp"),) * 3
    return jax.shard_map(body, mesh=mesh, in_specs=placed, out_specs=placed, check_vma=False)
```
